32 devices in a mesh: gx: 4 (over z), gy: 4 (over y, x), gz: 2 (over core).
Axes of the slice: x: 2, y: 2, z: 4, core: 2. Of those that a mesh axis runs over, the one named last changes fastest.
Arguments:
- cotangent: float32 [19, 32, 64, 256], P(None, 'gx', 'gy', 'gz'), may hold values from -6 to 6
- densities: float32 [3, 32, 64, 256], P(None, 'gx', 'gy', 'gz'), may hold values from 0.3 to 2.2
- velocities: float32 [3, 3, 32, 64, 256], P(None, None, 'gx', 'gy', 'gz'), may hold values from -0.16 to 0.16
- adhesion: float32 [32, 64, 256], P('gx', 'gy', 'gz'), may hold values from -1 to 1
- fluid: int32 [32, 64, 256], P('gx', 'gy', 'gz'), may hold values 0 or 1
Outputs:
- initial_cotangent: float32 [19, 32, 64, 256], P(None, 'gx', 'gy', 'gz')
- adhesion_grad: float32 [32, 64, 256], P('gx', 'gy', 'gz')
The draws below stay inside these ranges and needn't reach their ends.
All inputs are finite; a program needn't handle non-finite values. No bound on the sum of `fluid` on one device may be relied on, other than what follows from the above.
Results may differ from the reference program's by a relative error of at most 0.00002.
Values sent between devices are 32-bit elements; how exact they have to be, the bound alone decides.
No kernel may reach another device: no remote copies, remote signals or barrier semaphores. Data moves between devices by JAX's collectives and lax.ppermute only.
A program may use at most 64 MiB of HBM per device.

```python
import jax
import jax.numpy as jnp

STEPS = 3
NX = 32
NY = 64
NZ = 256


def place_ends(entries, own_key, least, largest):
    extent = entries.shape
    index_at = [jax.random.randint(jax.random.fold_in(own_key, axis), (), 0, extent[axis]) for axis in range(len(extent))]
    entries = entries.at[tuple(index_at)].set(least)
    longest = extent.index(max(extent))
    index_at[longest] = (index_at[longest] + 1) % extent[longest]
    return entries.at[tuple(index_at)].set(largest)


def block_levels(own_key, shape, shards, least, top_value):
    factor_of = 1.0
    for axis_at, shards_of in shards:
        steps = jax.random.uniform(jax.random.fold_in(jax.random.fold_in(own_key, 6), axis_at), (shards_of,), jnp.float32, least / len(shards), top_value / len(shards))
        factor_of = factor_of * jnp.repeat(jnp.exp(steps), shape[axis_at] // shards_of).reshape((-1,) + (1,) * (len(shape) - 1 - axis_at))
    return factor_of


def scatter_about(stream_key, dims, scale, limit, shards=(), held_as=jnp.bfloat16):
    drawn = jax.random.normal(stream_key, dims, jnp.float32) * scale
    if len(shards) > 0:
        drawn = block_levels(stream_key, dims, shards, -0.22, 0.18) * drawn
    return jnp.clip(drawn, min=-limit, max=limit).astype(held_as)


def setup_inputs(seed: int = 0) -> dict:
    streams_of = jax.random.split(jax.random.key(seed), 6)
    return {
        "cotangent": scatter_about(streams_of[0], (19, NX, NY, NZ), 1.0, 6.0, ((1, 4), (2, 4), (3, 2)), jnp.float32),
        "densities": jnp.clip(0.3 + 1.90000004 * jax.random.uniform(streams_of[1], (STEPS, NX, NY, NZ), jnp.float32) ** block_levels(streams_of[1], (STEPS, NX, NY, NZ), ((1, 4), (2, 4), (3, 2)), -0.2, 0.2), 0.3, 2.2),
        "velocities": scatter_about(streams_of[2], (STEPS, 3, NX, NY, NZ), 0.04, 0.16, ((2, 4), (3, 4), (4, 2)), jnp.float32),
        "adhesion": jnp.clip(jax.random.uniform(streams_of[3], (NX, NY, NZ), jnp.float32, -1.0, 1.0) * block_levels(streams_of[3], (NX, NY, NZ), ((0, 4), (1, 4), (2, 2)), -0.4, 0.0), -1.0, 1.0),
        "fluid": place_ends((jax.random.randint(streams_of[4], (NX, NY, NZ), 0, 10) < 7).astype(jnp.int32), jax.random.fold_in(streams_of[4], 1), 0, 1),
    }


DIRECTIONS = ((0, 0, 0), (1, 0, 0), (-1, 0, 0), (0, 1, 0), (0, -1, 0), (0, 0, 1), (0, 0, -1),
              (1, 1, 0), (-1, -1, 0), (1, -1, 0), (-1, 1, 0),
              (1, 0, 1), (-1, 0, -1), (1, 0, -1), (-1, 0, 1),
              (0, 1, 1), (0, -1, -1), (0, 1, -1), (0, -1, 1))
WEIGHTS = (1.0 / 3.0,) + (1.0 / 18.0,) * 6 + (1.0 / 36.0,) * 12
OPPOSITE = (0, 2, 1, 4, 3, 6, 5, 8, 7, 10, 9, 12, 11, 14, 13, 16, 15, 18, 17)
RELAX_TIME = 0.8
COUPLING = -5.0


def shifted(padded, offset):
    width = padded.shape[-3] - 2
    height = padded.shape[-2] - 2
    depth = padded.shape[-1] - 2
    return padded[..., 1 + offset[0]:1 + offset[0] + width, 1 + offset[1]:1 + offset[1] + height, 1 + offset[2]:1 + offset[2] + depth]


def adjoint_step(padded_cot, density_pad, gain_pad, velocity, fluid_pad, spread):
    incoming = padded_cot[:, 1:-1, 1:-1, 1:-1]
    own_cell = fluid_pad[1:-1, 1:-1, 1:-1]
    density = density_pad[1:-1, 1:-1, 1:-1]
    potential_pad = 1.0 - jnp.exp(-density_pad)
    potential = potential_pad[1:-1, 1:-1, 1:-1]
    passed = [incoming[0] * own_cell]
    attract = [jnp.zeros_like(density) for k in range(3)]
    for i in range(1, 19):
        offset = DIRECTIONS[i]
        beside = shifted(fluid_pad, offset)
        passed.append(own_cell * (beside * shifted(padded_cot[i], offset) + (1.0 - beside) * incoming[OPPOSITE[i]]))
        weighted = WEIGHTS[i] * (COUPLING * beside * shifted(potential_pad, offset) + (1.0 - beside) * shifted(gain_pad, offset))
        for k in range(3):
            if offset[k] != 0:
                attract[k] = attract[k] + offset[k] * weighted
    speed_sq = velocity[0] * velocity[0] + velocity[1] * velocity[1] + velocity[2] * velocity[2]
    density_bar = jnp.zeros_like(density)
    velo_bar = [jnp.zeros_like(density) for k in range(3)]
    for i in range(19):
        offset = DIRECTIONS[i]
        projected = offset[0] * velocity[0] + offset[1] * velocity[1] + offset[2] * velocity[2]
        e = passed[i] * (WEIGHTS[i] / RELAX_TIME)
        density_bar = density_bar + e * (1.0 + 3.0 * projected + 4.5 * projected * projected - 1.5 * speed_sq)
        scaled = e * density
        for k in range(3):
            velo_bar[k] = velo_bar[k] + scaled * (3.0 * offset[k] + 9.0 * projected * offset[k] - 3.0 * velocity[k])
    moment_bar = [velo_bar[k] / density for k in range(3)]
    density_bar = density_bar - (velo_bar[0] * velocity[0] + velo_bar[1] * velocity[1] + velo_bar[2] * velocity[2]) / density
    force_bar = [RELAX_TIME * moment_bar[k] for k in range(3)]
    potential_bar = -(force_bar[0] * attract[0] + force_bar[1] * attract[1] + force_bar[2] * attract[2])
    pushed = jnp.stack([potential * force_bar[k] * own_cell for k in range(3)])
    pushed_pad = spread(pushed)
    gathered = jnp.zeros_like(density)
    for i in range(1, 19):
        offset = DIRECTIONS[i]
        reverse = (-offset[0], -offset[1], -offset[2])
        for k in range(3):
            if offset[k] != 0:
                gathered = gathered + (WEIGHTS[i] * offset[k]) * shifted(pushed_pad[k], reverse)
    potential_bar = potential_bar - COUPLING * own_cell * gathered
    density_bar = density_bar + potential_bar * jnp.exp(-density)
    outgoing = []
    for i in range(19):
        offset = DIRECTIONS[i]
        total = (1.0 - 1.0 / RELAX_TIME) * passed[i] + density_bar
        for k in range(3):
            if offset[k] != 0:
                total = total + offset[k] * moment_bar[k]
        outgoing.append(own_cell * total)
    return jnp.stack(outgoing), -(1.0 - own_cell) * gathered


def pad_cells(values):
    return jnp.pad(values, ((0, 0), (1, 1), (1, 1), (1, 1)))


def reference(cotangent, densities, velocities, adhesion, fluid):
    gradient = jnp.zeros_like(adhesion)
    current = cotangent
    fluid_float = fluid.astype(jnp.float32)
    for s in reversed(range(STEPS)):
        states = pad_cells(jnp.stack([densities[s], adhesion, fluid_float]))
        current, gain_part = adjoint_step(pad_cells(current), states[0], states[1], velocities[s], states[2], pad_cells)
        gradient = gradient + gain_part
    return current, gradient
```

```python
import functools

import jax
import jax.numpy as jnp
from jax import lax
from jax.experimental import pallas as pl
from jax.experimental.pallas import tpu as pltpu
from jax.sharding import PartitionSpec as P

DIRECTIONS = (
    (0, 0, 0),
    (1, 0, 0),
    (-1, 0, 0),
    (0, 1, 0),
    (0, -1, 0),
    (0, 0, 1),
    (0, 0, -1),
    (1, 1, 0),
    (-1, -1, 0),
    (1, -1, 0),
    (-1, 1, 0),
    (1, 0, 1),
    (-1, 0, -1),
    (1, 0, -1),
    (-1, 0, 1),
    (0, 1, 1),
    (0, -1, -1),
    (0, 1, -1),
    (0, -1, 1),
)
OPPOSITE = (0, 2, 1, 4, 3, 6, 5, 8, 7, 10, 9, 12, 11, 14, 13, 16, 15, 18, 17)
RELAX_TIME = 0.8
COUPLING = -5.0
W_REST = 1.0 / 3.0 / RELAX_TIME
W_AXIS = 1.0 / 18.0 / RELAX_TIME
W_DIAG = 1.0 / 36.0 / RELAX_TIME
C18 = 1.0 / 18.0
C36 = 1.0 / 36.0

XP = tuple(i for i in range(19) if DIRECTIONS[i][0] == 1)
XM = tuple(i for i in range(19) if DIRECTIONS[i][0] == -1)
YP = tuple(i for i in range(19) if DIRECTIONS[i][1] == 1)
YM = tuple(i for i in range(19) if DIRECTIONS[i][1] == -1)
EDGE = {(1, 1): 7, (-1, -1): 8, (1, -1): 9, (-1, 1): 10}
PAD = 8
VMEM_LIMIT = 24 * 1024 * 1024
X_AXES = ("gx", "gz")


class Plan:
    def __init__(self, n_gx, n_gy, n_gz, block, steps):
        self.tiles = n_gz
        self.nx = block[0] // n_gz
        self.ny = block[1]
        self.lanes = block[2]
        self.steps = steps
        self.chain_x = n_gx * n_gz
        self.chain_y = n_gy
        self.n_gz = n_gz
        self.q_rho = 19
        self.q_vel = 19 + steps
        self.q_adh = 19 + 4 * steps
        self.q_fl = self.q_adh + 1
        self.nq = self.q_fl + 1
        self.n_state = steps + 2
        self.s_adh = steps
        self.s_fl = steps + 1
        self.rows = self.ny + 2 * PAD

    def padded(self, count):
        return (count, self.tiles, self.nx + 2, self.rows, self.lanes)

    def x_layout(self, last):
        at = 0 if last else 5 * self.ny
        out = {}
        if not last:
            out["own"] = at
            at += self.ny
        out["beyond"] = at
        at += self.ny
        out["ends"] = at
        out["rows"] = at + 8
        return out

    def y_layout(self, last):
        at = 0
        out = {}
        if not last:
            out["edges"] = 5 * self.nx
            at = 5 * self.nx + 2
            out["own"] = at
            at += self.nx + 2
        out["beyond"] = at
        at += self.nx + 2
        out["rows"] = -(-at // 8) * 8
        return out

    def input_y_layout(self):
        pops = self.n_state * (self.nx + 2)
        edges = pops + 5 * self.nx
        return {"pops": pops, "edges": edges, "rows": -(-(edges + 2) // 8) * 8}


def flag(cond, shape):
    return jnp.full(shape, cond.astype(jnp.int32), jnp.int32) == 1


def chain_place(axes, count):
    if axes == "gy":
        place = lax.axis_index("gy")
    else:
        place = lax.axis_index("gx") * lax.axis_size("gz") + lax.axis_index("gz")
    return place % 2 == 0, place < count - 1, place > 0


def pick(cond, one, other):
    return jnp.where(flag(cond, one.shape), one, other)


def halo_pair(place, first, second):
    even, has_plus, has_minus = place
    zero = jnp.zeros_like(first)
    plus = pick(has_plus, pick(even, first, second), zero)
    minus = pick(has_minus, pick(even, second, first), zero)
    return plus, minus


def z_shift(tiles, by):
    lanes = tiles[0].shape[-1]
    lane = lax.broadcasted_iota(jnp.int32, tiles[0].shape, len(tiles[0].shape) - 1)
    count = len(tiles)
    axis = len(tiles[0].shape) - 1
    if by == 1:
        rolled = [pltpu.roll(v, lanes - 1, axis) for v in tiles] + [jnp.zeros_like(tiles[0])]
        return [jnp.where(lane == lanes - 1, rolled[t + 1], rolled[t]) for t in range(count)]
    rolled = [jnp.zeros_like(tiles[0])] + [pltpu.roll(v, 1, axis) for v in tiles]
    return [jnp.where(lane == 0, rolled[t], rolled[t + 1]) for t in range(count)]


def each(fn, *lists):
    return [fn(*items) for items in zip(*lists)]


def split_kernel(plan, cot, dens, vel, adh, fluid, *rest):
    n = plan.n_gz
    outs = rest[:n]
    whole, sems = rest[n], rest[n + 1]
    me = lax.axis_index("gz")
    nx = plan.nx
    copies = []
    for k, d in enumerate(list(range(1, n)) + [0]):
        chunk = pl.ds(lax.rem(me + d, n) * nx, nx)
        out = outs[d]
        pairs = [
            (cot.at[:, chunk], out.at[0:19]),
            (dens.at[:, chunk], out.at[plan.q_rho : plan.q_rho + plan.steps]),
            (adh.at[chunk], out.at[plan.q_adh]),
            (fluid.at[chunk], whole.at[d]),
        ]
        for s in range(plan.steps):
            at = plan.q_vel + 3 * s
            pairs.append((vel.at[s, :, chunk], out.at[at : at + 3]))
        for j, (src, dst) in enumerate(pairs):
            copies.append(pltpu.make_async_copy(src, dst, sems.at[k, j]))
    for copy in copies:
        copy.start()
    for copy in copies:
        copy.wait()
    for d in range(n):
        outs[d][plan.q_fl] = whole[d].astype(jnp.float32)


def tile_of(plan, refs, t, index):
    me = lax.axis_index("gz")
    out = refs[0][index]
    for d in range(1, plan.n_gz):
        out = pick(lax.rem(me - t + plan.n_gz, plan.n_gz) == d, refs[d][index], out)
    return out


def state_index(plan, k):
    if k < plan.steps:
        return plan.q_rho + k
    return plan.q_adh if k == plan.s_adh else plan.q_fl


def input_x_kernel(plan, *refs):
    n = plan.n_gz
    parts, (out_a, out_b) = refs[:n], refs[n:]
    even = chain_place(X_AXES, plan.chain_x)[0]
    for t in range(plan.tiles):
        for j in range(5 + plan.n_state):
            up = XM[j] if j < 5 else state_index(plan, j - 5)
            down = XP[j] if j < 5 else state_index(plan, j - 5)
            plus = tile_of(plan, parts, t, (up, plan.nx - 1))
            minus = tile_of(plan, parts, t, (down, 0))
            out_a[j, t] = pick(even, plus, minus)
            out_b[j, t] = pick(even, minus, plus)


def input_y_kernel(plan, *refs):
    n = plan.n_gz
    parts = refs[:n]
    xr_a, xr_b, out_a, out_b, up, down = refs[n:]
    nx, ny = plan.nx, plan.ny
    lay = plan.input_y_layout()
    place_x = chain_place(X_AXES, plan.chain_x)
    even = chain_place("gy", plan.chain_y)[0]
    up[...] = jnp.zeros_like(up)
    down[...] = jnp.zeros_like(down)
    top = slice(ny - 1, ny)
    low = slice(0, 1)
    for t in range(plan.tiles):
        for k in range(plan.n_state):
            base = k * (nx + 2)
            plus, minus = halo_pair(place_x, xr_a[5 + k, t], xr_b[5 + k, t])
            for x in range(-1, nx + 1):
                if x < 0:
                    plane = minus
                elif x == nx:
                    plane = plus
                else:
                    plane = tile_of(plan, parts, t, (state_index(plan, k), x))
                r = base + x + 1
                up[t, r : r + 1] = plane[top]
                down[t, r : r + 1] = plane[low]
        for j in range(5):
            for x in range(nx):
                r = lay["pops"] + j * nx + x
                up[t, r : r + 1] = tile_of(plan, parts, t, (YM[j], x, top))
                down[t, r : r + 1] = tile_of(plan, parts, t, (YP[j], x, low))
        r = lay["edges"]
        for side, out, rows in ((-1, up, top), (1, down, low)):
            j = XM.index(EDGE[(-1, side)])
            out[t, r : r + 1] = halo_pair(place_x, xr_a[j, t], xr_b[j, t])[1][rows]
            j = XP.index(EDGE[(1, side)])
            out[t, r + 1 : r + 2] = halo_pair(place_x, xr_a[j, t], xr_b[j, t])[0][rows]
        out_a[t] = pick(even, up[t], down[t])
        out_b[t] = pick(even, down[t], up[t])


def fill_inputs(plan, parts, xr_a, xr_b, yr_a, yr_b, state, apad):
    nx, ny = plan.nx, plan.ny
    lay = plan.input_y_layout()
    place_x = chain_place(X_AXES, plan.chain_x)
    place_y = chain_place("gy", plan.chain_y)
    own = slice(PAD, PAD + ny)
    first, last = slice(PAD - 1, PAD), slice(PAD + ny, PAD + ny + 1)
    for t in range(plan.tiles):
        y_plus, y_minus = halo_pair(place_y, yr_a[t], yr_b[t])
        for k in range(plan.n_state):
            plus, minus = halo_pair(place_x, xr_a[5 + k, t], xr_b[5 + k, t])
            for x in range(-1, nx + 1):
                if x < 0:
                    plane = minus
                elif x == nx:
                    plane = plus
                else:
                    plane = tile_of(plan, parts, t, (state_index(plan, k), x))
                r = k * (nx + 2) + x + 1
                state[k, t, x + 1, own] = plane
                state[k, t, x + 1, first] = y_minus[r : r + 1]
                state[k, t, x + 1, last] = y_plus[r : r + 1]
        fl = plan.s_fl
        for x in range(nx):
            mask = state[fl, t, x + 1, own]
            for i in range(19):
                apad[i, t, x + 1, own] = mask * tile_of(plan, parts, t, (i, x))
            mask_first = state[fl, t, x + 1, first]
            mask_last = state[fl, t, x + 1, last]
            for j in range(5):
                r = lay["pops"] + j * nx + x
                apad[YP[j], t, x + 1, last] = mask_last * y_plus[r : r + 1]
                apad[YM[j], t, x + 1, first] = mask_first * y_minus[r : r + 1]
        for j in range(5):
            plus, minus = halo_pair(place_x, xr_a[j, t], xr_b[j, t])
            apad[XP[j], t, nx + 1, own] = state[fl, t, nx + 1, own] * plus
            apad[XM[j], t, 0, own] = state[fl, t, 0, own] * minus
        r = lay["edges"]
        for side, rows, msg in ((1, last, y_plus), (-1, first, y_minus)):
            apad[EDGE[(-1, side)], t, 0, rows] = state[fl, t, 0, rows] * msg[r : r + 1]
            apad[EDGE[(1, side)], t, nx + 1, rows] = state[fl, t, nx + 1, rows] * msg[r + 1 : r + 2]


def complete_back(plan, last_phase, ksum, yr_a, yr_b, total):
    nx, ny = plan.nx, plan.ny
    lay = plan.y_layout(last_phase)
    place_y = chain_place("gy", plan.chain_y)
    total[...] = ksum[...]
    for t in range(plan.tiles):
        plus, minus = halo_pair(place_y, yr_a[t], yr_b[t])
        for x in range(nx + 2):
            r = lay["beyond"] + x
            rows = slice(PAD + ny - 1, PAD + ny)
            total[t, x, rows] = total[t, x, rows] + plus[r : r + 1]
            rows = slice(PAD, PAD + 1)
            total[t, x, rows] = total[t, x, rows] + minus[r : r + 1]
            if not last_phase:
                r = lay["own"] + x
                rows = slice(PAD + ny, PAD + ny + 1)
                total[t, x, rows] = total[t, x, rows] + plus[r : r + 1]
                rows = slice(PAD - 1, PAD)
                total[t, x, rows] = total[t, x, rows] + minus[r : r + 1]


def fill_next(plan, s, state, a_in, ksum, xr_a, xr_b, yr_a, yr_b, grad_in, grad_out, total, apad):
    nx, ny = plan.nx, plan.ny
    lay = plan.y_layout(False)
    place_x = chain_place(X_AXES, plan.chain_x)
    place_y = chain_place("gy", plan.chain_y)
    own = slice(PAD, PAD + ny)
    first, last = slice(PAD - 1, PAD), slice(PAD + ny, PAD + ny + 1)
    complete_back(plan, False, ksum, yr_a, yr_b, total)

    def extra(t, x, rows):
        mask = state[plan.s_fl, t, x + 1, rows]
        rho = state[s + 1, t, x + 1, rows]
        return (-COUPLING) * mask * jnp.exp(-rho) * total[t, x + 1, rows]

    for t in range(plan.tiles):
        y_plus, y_minus = halo_pair(place_y, yr_a[t], yr_b[t])
        for x in range(nx):
            more = extra(t, x, own)
            part = (1.0 - state[plan.s_fl, t, x + 1, own]) * total[t, x + 1, own]
            grad_out[t, x] = -part if grad_in is None else grad_in[t, x] - part
            for i in range(19):
                apad[i, t, x + 1, own] = a_in[i, t, x] + more
            more_first, more_last = extra(t, x, first), extra(t, x, last)
            for j in range(5):
                r = j * nx + x
                apad[YP[j], t, x + 1, last] = y_plus[r : r + 1] + more_last
                apad[YM[j], t, x + 1, first] = y_minus[r : r + 1] + more_first
        more_plus, more_minus = extra(t, nx, own), extra(t, -1, own)
        for j in range(5):
            rows = slice(j * ny, (j + 1) * ny)
            plus, minus = halo_pair(place_x, xr_a[t, rows], xr_b[t, rows])
            apad[XP[j], t, nx + 1, own] = plus + more_plus
            apad[XM[j], t, 0, own] = minus + more_minus
        r = lay["edges"]
        for side, rows, msg in ((1, last, y_plus), (-1, first, y_minus)):
            apad[EDGE[(-1, side)], t, 0, rows] = msg[r : r + 1] + extra(t, -1, rows)
            apad[EDGE[(1, side)], t, nx + 1, rows] = msg[r + 1 : r + 2] + extra(t, nx, rows)


def fill_phi(plan, s, state, phi):
    for t in range(plan.tiles):
        for x in range(plan.nx + 2):
            mask = state[plan.s_fl, t, x]
            psi = 1.0 - jnp.exp(-state[s, t, x])
            phi[t, x] = COUPLING * mask * psi + (1.0 - mask) * state[plan.s_adh, t, x]


def force_at(plan, phi, x, rows):
    tiles = range(plan.tiles)

    def at(dx, dy):
        return [phi[t, x + 1 + dx, rows.start + dy : rows.stop + dy] for t in tiles]

    sub, add = (lambda a, b: a - b), (lambda a, b: a + b)
    xp, xm, yp, ym, mid = at(1, 0), at(-1, 0), at(0, 1), at(0, -1), at(0, 0)
    pp, pm, mp, mm = at(1, 1), at(1, -1), at(-1, 1), at(-1, -1)
    dx, dy = each(sub, xp, xm), each(sub, yp, ym)
    zd = each(lambda m, a, b, c, d: C18 * m + C36 * ((a + b) + (c + d)), mid, xp, xm, yp, ym)
    dxu, dxd, dyu, dyd = z_shift(dx, 1), z_shift(dx, -1), z_shift(dy, 1), z_shift(dy, -1)
    px = each(
        lambda d, u, w, a, b, c, e: C18 * d + C36 * ((u + w) + ((a - c) + (b - e))),
        dx, dxu, dxd, pp, pm, mp, mm,
    )
    py = each(
        lambda d, u, w, a, b, c, e: C18 * d + C36 * ((u + w) + ((a - b) + (c - e))),
        dy, dyu, dyd, pp, pm, mp, mm,
    )
    pz = each(sub, z_shift(zd, 1), z_shift(zd, -1))
    return px, py, pz


def cells(plan, s, state, solid, fresh, vel, phi, apad, a_out, vpad, kept):
    nx, ny = plan.nx, plan.ny
    tiles = range(plan.tiles)
    for x in range(nx):
        for r0 in range(0, ny, 8):
            own = slice(PAD + r0, PAD + r0 + 8)
            here = slice(r0, r0 + 8)
            b = [[apad[0, t, x + 1, own] for t in tiles]]
            for i in range(1, 19):
                cx, cy, cz = DIRECTIONS[i]
                rows = slice(own.start + cy, own.stop + cy)
                came = [apad[i, t, x + 1 + cx, rows] for t in tiles]
                if cz:
                    came = z_shift(came, cz)
                if fresh:
                    open_to = [state[plan.s_fl, t, x + 1 + cx, rows] for t in tiles]
                    if cz:
                        open_to = z_shift(open_to, cz)
                    wall = [1.0 - v for v in open_to]
                    for t in tiles:
                        solid[i - 1, t, x, here] = wall[t]
                else:
                    wall = [solid[i - 1, t, x, here] for t in tiles]
                back = [apad[OPPOSITE[i], t, x + 1, own] for t in tiles]
                b.append(each(lambda c, w, o: c + w * o, came, wall, back))
            force = force_at(plan, phi, x, own)
            for t in tiles:
                g = [v[t] for v in b]
                sm = {i: g[i] + g[i + 1] for i in range(1, 19, 2)}
                df = {i: g[i] - g[i + 1] for i in range(1, 19, 2)}
                sxy, sxz, syz = sm[7] + sm[9], sm[11] + sm[13], sm[15] + sm[17]
                ux, uy, uz = vel(t, 0, x, here), vel(t, 1, x, here), vel(t, 2, x, here)
                m1x = W_AXIS * df[1] + W_DIAG * ((df[7] + df[9]) + (df[11] + df[13]))
                m1y = W_AXIS * df[3] + W_DIAG * ((df[7] - df[9]) + (df[15] + df[17]))
                m1z = W_AXIS * df[5] + W_DIAG * ((df[11] - df[13]) + (df[15] - df[17]))
                mxx = W_AXIS * sm[1] + W_DIAG * (sxy + sxz)
                myy = W_AXIS * sm[3] + W_DIAG * (sxy + syz)
                mzz = W_AXIS * sm[5] + W_DIAG * (sxz + syz)
                mxy = W_DIAG * (sm[7] - sm[9])
                mxz = W_DIAG * (sm[11] - sm[13])
                myz = W_DIAG * (sm[15] - sm[17])
                m0 = W_REST * g[0] + W_AXIS * ((sm[1] + sm[3]) + sm[5]) + W_DIAG * ((sxy + sxz) + syz)
                vx = mxx * ux + mxy * uy + mxz * uz
                vy = mxy * ux + myy * uy + myz * uz
                vz = mxz * ux + myz * uy + mzz * uz
                mbx = 3.0 * (m1x - ux * m0) + 9.0 * vx
                mby = 3.0 * (m1y - uy * m0) + 9.0 * vy
                mbz = 3.0 * (m1z - uz * m0) + 9.0 * vz
                usq = ux * ux + uy * uy + uz * uz
                rhobar = m0 * (1.0 + 1.5 * usq) - 4.5 * (ux * vx + uy * vy + uz * vz)
                fade = jnp.exp(-state[s, t, x + 1, own])
                mask = state[plan.s_fl, t, x + 1, own]
                pull = mbx * force[0][t] + mby * force[1][t] + mbz * force[2][t]
                rhobar = rhobar - RELAX_TIME * pull * fade
                scale = RELAX_TIME * mask * (1.0 - fade)
                vpad[0, t, x, own] = scale * mbx
                vpad[1, t, x, own] = scale * mby
                vpad[2, t, x, own] = scale * mbz
                rb, mx, my, mz = mask * rhobar, mask * mbx, mask * mby, mask * mbz
                damp = (1.0 - 1.0 / RELAX_TIME) * mask
                a_out(0, t, x, here, rb + damp * g[0])
                for i in range(1, 19, 2):
                    cx, cy, cz = DIRECTIONS[i]
                    along = None
                    for c, m in ((cx, mx), (cy, my), (cz, mz)):
                        if c == 1:
                            along = m if along is None else along + m
                        elif c == -1:
                            along = along - m
                    a_out(i, t, x, here, (rb + along) + damp * g[i])
                    a_out(i + 1, t, x, here, (rb - along) + damp * g[i + 1])


def sums_of_back(plan, vpad, kext):
    nx, ny = plan.nx, plan.ny
    tiles = range(plan.tiles)
    add = lambda a, b: a + b
    chunks = [slice(PAD + r, PAD + r + 8) for r in range(0, ny, 8)]
    chunks += [slice(PAD - 1, PAD), slice(PAD + ny, PAD + ny + 1)]
    for x in range(-1, nx + 1):
        for rows in chunks:

            def at(k, dx, dy):
                if not 0 <= x + dx < nx:
                    return None
                return [vpad[k, t, x + dx, rows.start + dy : rows.stop + dy] for t in tiles]

            def combine(a, b, sign):
                if a is None and b is None:
                    return None
                if b is None:
                    return a
                if a is None:
                    return b if sign > 0 else [-v for v in b]
                return each((lambda p, q: p + q) if sign > 0 else (lambda p, q: p - q), a, b)

            def times(c, a):
                return None if a is None else [c * v for v in a]

            dx0 = combine(at(0, 1, 0), at(0, -1, 0), -1)
            dxs = combine(
                combine(at(0, 1, 1), at(0, -1, 1), -1), combine(at(0, 1, -1), at(0, -1, -1), -1), 1
            )
            dy0 = combine(at(1, 0, 1), at(1, 0, -1), -1)
            dys = combine(
                combine(at(1, 1, 1), at(1, 1, -1), -1), combine(at(1, -1, 1), at(1, -1, -1), -1), 1
            )
            zsum = times(C36, combine(dx0, dy0, 1))
            side = combine(combine(at(2, 1, 0), at(2, -1, 0), 1), combine(at(2, 0, 1), at(2, 0, -1), 1), 1)
            zdif = combine(times(C18, at(2, 0, 0)), times(C36, side), 1)
            flat = combine(times(C18, combine(dx0, dy0, 1)), times(C36, combine(dxs, dys, 1)), 1)
            up = z_shift(combine(zsum, zdif, 1), 1)
            down = z_shift(combine(zsum, zdif, -1), -1)
            for t in tiles:
                kext[t, x + 1, rows] = -(flat[t] + (up[t] + down[t]))


def pack_x(plan, last_phase, a_of, kext, out_a, out_b):
    nx, ny = plan.nx, plan.ny
    lay = plan.x_layout(last_phase)
    even = chain_place(X_AXES, plan.chain_x)[0]
    own = slice(PAD, PAD + ny)

    def put(t, rows, plus, minus):
        out_a[t, rows] = pick(even, plus, minus)
        out_b[t, rows] = pick(even, minus, plus)

    for t in range(plan.tiles):
        if not last_phase:
            for j in range(5):
                put(t, slice(j * ny, (j + 1) * ny), a_of(XM[j], t, nx - 1), a_of(XP[j], t, 0))
            put(t, slice(lay["own"], lay["own"] + ny), kext[t, nx, own], kext[t, 1, own])
        put(t, slice(lay["beyond"], lay["beyond"] + ny), kext[t, nx + 1, own], kext[t, 0, own])
        r = lay["ends"]
        blank = jnp.zeros((8, plan.lanes), jnp.float32)
        out_a[t, r : r + 8] = blank
        out_b[t, r : r + 8] = blank
        for j, row in enumerate((PAD - 1, PAD + ny)):
            rows = slice(row, row + 1)
            put(t, slice(r + j, r + j + 1), kext[t, nx + 1, rows], kext[t, 0, rows])
            if not last_phase:
                put(t, slice(r + 2 + j, r + 3 + j), kext[t, nx, rows], kext[t, 1, rows])


def pack_rows(plan, a_of_row, up, down):
    for t in range(plan.tiles):
        up[t] = jnp.zeros_like(up[t])
        down[t] = jnp.zeros_like(down[t])
        for j in range(5):
            for x in range(plan.nx):
                r = j * plan.nx + x
                up[t, r : r + 1] = a_of_row(YM[j], t, x, plan.ny - 1)
                down[t, r : r + 1] = a_of_row(YP[j], t, x, 0)


def finish_step(plan, last_phase, a_ref, vpad, kext, out_a, out_b, up, down):
    sums_of_back(plan, vpad, kext)
    pack_x(plan, last_phase, lambda i, t, x: a_ref[i, t, x], kext, out_a, out_b)
    if not last_phase:
        pack_rows(plan, lambda i, t, x, row: a_ref[i, t, x, row : row + 1], up, down)


def blank_rows(plan, ref):
    blank = jnp.zeros((PAD, plan.lanes), jnp.float32)
    for k in range(3):
        for t in range(plan.tiles):
            for x in range(plan.nx):
                ref[k, t, x, 0:PAD] = blank
                ref[k, t, x, PAD + plan.ny :] = blank


def first_kernel(plan, *refs):
    n = plan.n_gz
    parts = refs[:n]
    xr_a, xr_b, yr_a, yr_b = refs[n : n + 4]
    state, solid, vels, a_ref, kext, out_a, out_b, up, down, apad, phi, vpad = refs[n + 4 :]
    s = plan.steps - 1
    last_phase = s == 0
    fill_inputs(plan, parts, xr_a, xr_b, yr_a, yr_b, state, apad)
    for t in range(plan.tiles):
        for k in range(3 * (plan.steps - 1)):
            vels[k, t] = tile_of(plan, parts, t, (plan.q_vel + k,))
    fill_phi(plan, s, state, phi)
    blank_rows(plan, vpad)

    def vel(t, k, x, here):
        return tile_of(plan, parts, t, (plan.q_vel + 3 * s + k, x, here))

    def a_out(i, t, x, here, value):
        a_ref[i, t, x, here] = value

    cells(plan, s, state, solid, True, vel, phi, apad, a_out, vpad, None)
    finish_step(plan, last_phase, a_ref, vpad, kext, out_a, out_b, up, down)


def next_kernel(plan, s, has_grad, *refs):
    refs = list(refs)
    take = lambda k: [refs.pop(0) for _ in range(k)]
    last_phase = s == 0
    state, solid, vels, a_in, ksum, xr_a, xr_b, yr_a, yr_b = take(9)
    grad_in = take(1)[0] if has_grad else None
    if last_phase:
        tiles_out = take(plan.n_gz)
        kext, out_a, out_b, grad_out, apad, phi, vpad, total, a_ref = take(9)
        up = down = None
    else:
        a_ref, kext, out_a, out_b, up, down, grad_out, apad, phi, vpad, total = take(11)
    fill_next(plan, s, state, a_in, ksum, xr_a, xr_b, yr_a, yr_b, grad_in, grad_out, total, apad)
    fill_phi(plan, s, state, phi)
    blank_rows(plan, vpad)

    def vel(t, k, x, here):
        return vels[3 * s + k, t, x, here]

    def a_out(i, t, x, here, value):
        if last_phase:
            a_ref[t, i, x, here] = value
        else:
            a_ref[i, t, x, here] = value

    cells(plan, s, state, solid, False, vel, phi, apad, a_out, vpad, None)
    finish_step(plan, last_phase, a_ref, vpad, kext, out_a, out_b, up, down)
    if last_phase:
        me = lax.axis_index("gz")
        for d in range(plan.n_gz):
            tiles_out[d][...] = a_ref[lax.rem(me + d, plan.n_gz)]


def y_kernel(plan, last_phase, *refs):
    if last_phase:
        kext, xr_a, xr_b, ksum, out_a, out_b, up, down = refs
        up[...] = jnp.zeros_like(up)
        down[...] = jnp.zeros_like(down)
    else:
        kext, xr_a, xr_b, up_in, down_in, ksum, out_a, out_b, up, down = refs
        up[...] = up_in[...]
        down[...] = down_in[...]
    nx, ny = plan.nx, plan.ny
    lay_x, lay_y = plan.x_layout(last_phase), plan.y_layout(last_phase)
    place_x = chain_place(X_AXES, plan.chain_x)
    even = chain_place("gy", plan.chain_y)[0]
    own = slice(PAD, PAD + ny)
    ksum[...] = kext[...]
    for t in range(plan.tiles):

        def add(x, rows, msg_rows, side):
            part = halo_pair(place_x, xr_a[t, msg_rows], xr_b[t, msg_rows])[side]
            ksum[t, x + 1, rows] = ksum[t, x + 1, rows] + part

        for x, side in ((nx - 1, 0), (0, 1)):
            add(x, own, slice(lay_x["beyond"], lay_x["beyond"] + ny), side)
            for j, row in enumerate((PAD - 1, PAD + ny)):
                r = lay_x["ends"] + j
                add(x, slice(row, row + 1), slice(r, r + 1), side)
        if not last_phase:
            for x, side in ((nx, 0), (-1, 1)):
                add(x, own, slice(lay_x["own"], lay_x["own"] + ny), side)
                for j, row in enumerate((PAD - 1, PAD + ny)):
                    r = lay_x["ends"] + 2 + j
                    add(x, slice(row, row + 1), slice(r, r + 1), side)
            r = lay_y["edges"]
            for side, out, row in ((-1, up, ny - 1), (1, down, 0)):
                j = XM.index(EDGE[(-1, side)]) * ny + row
                out[t, r : r + 1] = halo_pair(place_x, xr_a[t, j : j + 1], xr_b[t, j : j + 1])[1]
                j = XP.index(EDGE[(1, side)]) * ny + row
                out[t, r + 1 : r + 2] = halo_pair(place_x, xr_a[t, j : j + 1], xr_b[t, j : j + 1])[0]
        for x in range(nx + 2):
            r = lay_y["beyond"] + x
            up[t, r : r + 1] = ksum[t, x, PAD + ny : PAD + ny + 1]
            down[t, r : r + 1] = ksum[t, x, PAD - 1 : PAD]
            if not last_phase:
                r = lay_y["own"] + x
                up[t, r : r + 1] = ksum[t, x, PAD + ny - 1 : PAD + ny]
                down[t, r : r + 1] = ksum[t, x, PAD : PAD + 1]
        out_a[t] = pick(even, up[t], down[t])
        out_b[t] = pick(even, down[t], up[t])


def close_kernel(plan, state, ksum, yr_a, yr_b, grad_in, *rest):
    n = plan.n_gz
    outs, (total, both) = rest[:n], rest[n:]
    own = slice(PAD, PAD + plan.ny)
    complete_back(plan, True, ksum, yr_a, yr_b, total)
    for t in range(plan.tiles):
        for x in range(plan.nx):
            mask = state[plan.s_fl, t, x + 1, own]
            rho = state[0, t, x + 1, own]
            back = total[t, x + 1, own]
            both[t, 0, x] = (-COUPLING) * mask * jnp.exp(-rho) * back
            both[t, 1, x] = grad_in[t, x] - (1.0 - mask) * back
    me = lax.axis_index("gz")
    for d in range(n):
        outs[d][...] = both[lax.rem(me + d, n)]


def join_kernel(plan, *refs):
    n = plan.n_gz
    a_parts, r_parts, (out, grad) = refs[:n], refs[n : 2 * n], refs[2 * n :]
    me = lax.axis_index("gz")
    for d in range(n):
        chunk = pl.ds(lax.rem(me - d + n, n) * plan.nx, plan.nx)
        for i in range(19):
            out[i, chunk] = a_parts[d][i] + r_parts[d][0]
        grad[chunk] = r_parts[d][1]


def swaps(count):
    one = [(i, i ^ 1) for i in range(count)]
    two = [(i, (i + 1) % count if i % 2 else (i - 1) % count) for i in range(count)]
    return one, two


def swap_along(axes, count, first, second):
    one, two = swaps(count)
    return lax.ppermute(first, axes, one), lax.ppermute(second, axes, two)


def call(kernel, name, outs, scratch, args, flops, in_hbm=False):
    spec = pl.BlockSpec(memory_space=pl.ANY if in_hbm else pltpu.VMEM)
    return pl.pallas_call(
        kernel,
        name=name,
        out_shape=tuple(jax.ShapeDtypeStruct(shape, jnp.float32) for shape in outs),
        in_specs=[spec] * len(args),
        out_specs=tuple(pl.BlockSpec(memory_space=pltpu.VMEM) for _ in outs),
        scratch_shapes=scratch,
        cost_estimate=pl.CostEstimate(flops=flops, bytes_accessed=0, transcendentals=0),
        compiler_params=pltpu.CompilerParams(vmem_limit_bytes=VMEM_LIMIT),
    )(*args)


def per_device(cotangent, densities, velocities, adhesion, fluid):
    n = lax.axis_size("gz")
    plan = Plan(lax.axis_size("gx"), lax.axis_size("gy"), n, adhesion.shape, densities.shape[0])
    tiles, nx, ny, lanes, steps = plan.tiles, plan.nx, plan.ny, plan.lanes, plan.steps
    f32 = jnp.float32
    field = (tiles, nx, ny, lanes)
    padded = plan.padded(1)[1:]

    def along_x(first, second):
        return swap_along(X_AXES, plan.chain_x, first, second)

    def along_y(first, second):
        return swap_along("gy", plan.chain_y, first, second)

    def within_gz(parts):
        return [parts[0]] + [
            lax.ppermute(parts[d], "gz", [(i, (i + d) % n) for i in range(n)]) for d in range(1, n)
        ]

    part = (plan.nq, nx, ny, lanes)
    parts = call(
        functools.partial(split_kernel, plan),
        "split",
        [part] * n,
        [pltpu.VMEM((n, nx, ny, lanes), jnp.int32), pltpu.SemaphoreType.DMA((n, 4 + steps))],
        (cotangent, densities, velocities, adhesion, fluid),
        1000,
        in_hbm=True,
    )
    parts = within_gz(parts)

    msg = (5 + plan.n_state, tiles, ny, lanes)
    xr = along_x(*call(functools.partial(input_x_kernel, plan), "input_x", [msg] * 2, [], parts, 1000))
    msg = (tiles, plan.input_y_layout()["rows"], lanes)
    buffers = [pltpu.VMEM(msg, f32)] * 2
    yr = along_y(
        *call(functools.partial(input_y_kernel, plan), "input_y", [msg] * 2, buffers, (*parts, *xr), 1000)
    )

    work = [pltpu.VMEM(plan.padded(19), f32), pltpu.VMEM(padded, f32)]
    work.append(pltpu.VMEM((3, tiles, nx, plan.rows, lanes), f32))

    def x_message(last_phase):
        return (tiles, plan.x_layout(last_phase)["rows"], lanes)

    def y_message(last_phase):
        return (tiles, plan.y_layout(last_phase)["rows"], lanes)

    pops = (19, *field)
    outs = [plan.padded(plan.n_state), (18, *field), (3 * (steps - 1), *field), pops, padded]
    outs += [x_message(False)] * 2 + [y_message(False)] * 2
    state, solid, vels, a, kext, xa, xb, up, down = call(
        functools.partial(first_kernel, plan), "first", outs, work, (*parts, *xr, *yr), 100000
    )
    grad = None
    for s in reversed(range(steps - 1)):
        xr = along_x(xa, xb)
        msg = y_message(False)
        ksum, ya, yb = call(
            functools.partial(y_kernel, plan, False),
            f"rows_{s}",
            [padded, msg, msg],
            [pltpu.VMEM(msg, f32)] * 2,
            (kext, *xr, up, down),
            1000,
        )
        yr = along_y(ya, yb)
        args = [state, solid, vels, a, ksum, *xr, *yr]
        if grad is not None:
            args.append(grad)
        scratch = work + [pltpu.VMEM(padded, f32)]
        if s > 0:
            outs = [pops, padded] + [x_message(False)] * 2 + [y_message(False)] * 2 + [field]
        else:
            outs = [(19, nx, ny, lanes)] * n + [padded] + [x_message(True)] * 2 + [field]
            scratch = scratch + [pltpu.VMEM((tiles, 19, nx, ny, lanes), f32)]
        res = call(
            functools.partial(next_kernel, plan, s, grad is not None), f"next_{s}", outs, scratch, args, 100000
        )
        if s > 0:
            a, kext, xa, xb, up, down, grad = res
        else:
            a_parts, (kext, xa, xb, grad) = res[:n], res[n:]

    a_parts = within_gz(a_parts)
    xr = along_x(xa, xb)
    msg = y_message(True)
    ksum, ya, yb = call(
        functools.partial(y_kernel, plan, True),
        "rows_end",
        [padded, msg, msg],
        [pltpu.VMEM(msg, f32)] * 2,
        (kext, *xr),
        1000,
    )
    yr = along_y(ya, yb)
    both = (2, nx, ny, lanes)
    r_parts = call(
        functools.partial(close_kernel, plan),
        "close",
        [both] * n,
        [pltpu.VMEM(padded, f32), pltpu.VMEM((tiles, *both), f32)],
        (state, ksum, *yr, grad),
        1000,
    )
    r_parts = within_gz(r_parts)
    out, gradient = call(
        functools.partial(join_kernel, plan),
        "join",
        [cotangent.shape, adhesion.shape],
        [],
        (*a_parts, *r_parts),
        1000,
    )
    return out, gradient


def solution(mesh):
    return jax.shard_map(
        per_device,
        mesh=mesh,
        in_specs=(
            P(None, "gx", "gy", "gz"),
            P(None, "gx", "gy", "gz"),
            P(None, None, "gx", "gy", "gz"),
            P("gx", "gy", "gz"),
            P("gx", "gy", "gz"),
        ),
        out_specs=(P(None, "gx", "gy", "gz"), P("gx", "gy", "gz")),
        check_vma=False,
    )
```

```python
import functools

import jax
import jax.numpy as jnp
from jax import lax
from jax.experimental import pallas as pl
from jax.experimental.pallas import tpu as pltpu
from jax.sharding import PartitionSpec as P

DIRECTIONS = (
    (0, 0, 0),
    (1, 0, 0),
    (-1, 0, 0),
    (0, 1, 0),
    (0, -1, 0),
    (0, 0, 1),
    (0, 0, -1),
    (1, 1, 0),
    (-1, -1, 0),
    (1, -1, 0),
    (-1, 1, 0),
    (1, 0, 1),
    (-1, 0, -1),
    (1, 0, -1),
    (-1, 0, 1),
    (0, 1, 1),
    (0, -1, -1),
    (0, 1, -1),
    (0, -1, 1),
)
OPPOSITE = (0, 2, 1, 4, 3, 6, 5, 8, 7, 10, 9, 12, 11, 14, 13, 16, 15, 18, 17)
RELAX_TIME = 0.8
COUPLING = -5.0
W_REST = 1.0 / 3.0 / RELAX_TIME
W_AXIS = 1.0 / 18.0 / RELAX_TIME
W_DIAG = 1.0 / 36.0 / RELAX_TIME
C18 = 1.0 / 18.0
C36 = 1.0 / 36.0

XP = tuple(i for i in range(19) if DIRECTIONS[i][0] == 1)
XM = tuple(i for i in range(19) if DIRECTIONS[i][0] == -1)
YP = tuple(i for i in range(19) if DIRECTIONS[i][1] == 1)
YM = tuple(i for i in range(19) if DIRECTIONS[i][1] == -1)
EDGE = {(1, 1): 7, (-1, -1): 8, (1, -1): 9, (-1, 1): 10}
PAD = 8
VMEM_LIMIT = 24 * 1024 * 1024
X_AXES = ("gx", "gz")


class Plan:
    def __init__(self, n_gx, n_gy, n_gz, block, steps):
        self.tiles = n_gz
        self.nx = block[0] // n_gz
        self.ny = block[1]
        self.lanes = block[2]
        self.steps = steps
        self.chain_x = n_gx * n_gz
        self.chain_y = n_gy
        self.n_gx, self.n_gy, self.n_gz = n_gx, n_gy, n_gz
        self.q_rho = 19
        self.q_vel = 19 + steps
        self.q_adh = 19 + 4 * steps
        self.q_fl = self.q_adh + 1
        self.nq = self.q_fl + 1
        self.n_state = steps + 2
        self.s_adh = steps
        self.s_fl = steps + 1
        self.rows = self.ny + 2 * PAD
        self.in_rows = -(-(5 + self.n_state) // 8) * 8
        self.in_ends = -(-(2 * self.n_state + 2) // 8) * 8

    def padded(self, count):
        return (count, self.tiles, self.nx + 2, self.rows, self.lanes)

    def x_layout(self, last):
        at = 0 if last else 5 * self.ny
        out = {}
        if not last:
            out["own"] = at
            at += self.ny
        out["beyond"] = at
        at += self.ny
        out["ends"] = at
        out["rows"] = at + 8
        return out

    def y_layout(self, last):
        at = 0
        out = {}
        if not last:
            out["edges"] = 5 * self.nx
            at = 5 * self.nx + 2
            out["own"] = at
            at += self.nx + 2
        out["beyond"] = at
        at += self.nx + 2
        out["rows"] = -(-at // 8) * 8
        return out


def flag(cond, shape):
    return jnp.full(shape, cond.astype(jnp.int32), jnp.int32) == 1


def chain_place(axes, count):
    if axes == "gy":
        place = lax.axis_index("gy")
    else:
        place = lax.axis_index("gx") * lax.axis_size("gz") + lax.axis_index("gz")
    return place % 2 == 0, place < count - 1, place > 0


def pick(cond, one, other):
    return jnp.where(flag(cond, one.shape), one, other)


def halo_pair(place, first, second):
    even, has_plus, has_minus = place
    zero = jnp.zeros_like(first)
    plus = pick(has_plus, pick(even, first, second), zero)
    minus = pick(has_minus, pick(even, second, first), zero)
    return plus, minus


def z_shift(tiles, by):
    lanes = tiles[0].shape[-1]
    lane = lax.broadcasted_iota(jnp.int32, tiles[0].shape, len(tiles[0].shape) - 1)
    count = len(tiles)
    axis = len(tiles[0].shape) - 1
    if by == 1:
        rolled = [pltpu.roll(v, lanes - 1, axis) for v in tiles] + [jnp.zeros_like(tiles[0])]
        return [jnp.where(lane == lanes - 1, rolled[t + 1], rolled[t]) for t in range(count)]
    rolled = [jnp.zeros_like(tiles[0])] + [pltpu.roll(v, 1, axis) for v in tiles]
    return [jnp.where(lane == 0, rolled[t], rolled[t + 1]) for t in range(count)]


def each(fn, *lists):
    return [fn(*items) for items in zip(*lists)]


def split_kernel(plan, cot, dens, vel, adh, fluid, *rest):
    n = plan.n_gz
    outs, (out_a, out_b) = rest[:n], rest[n : n + 2]
    whole, up, down, sems = rest[n + 2 :]
    me = lax.axis_index("gz")
    nx, ny = plan.nx, plan.ny
    copies = []
    for d in range(n):
        chunk = pl.ds(lax.rem(me + d, n) * nx, nx)
        out = outs[d]
        pairs = [
            (cot.at[:, chunk], out.at[0:19]),
            (dens.at[:, chunk], out.at[plan.q_rho : plan.q_rho + plan.steps]),
            (adh.at[chunk], out.at[plan.q_adh]),
            (fluid.at[chunk], whole.at[d]),
        ]
        for s in range(plan.steps):
            at = plan.q_vel + 3 * s
            pairs.append((vel.at[s, :, chunk], out.at[at : at + 3]))
        for k, (src, dst) in enumerate(pairs):
            copies.append(pltpu.make_async_copy(src, dst, sems.at[d, k]))
    for copy in copies:
        copy.start()
    up[...] = jnp.zeros_like(up)
    down[...] = jnp.zeros_like(down)
    for copy in copies:
        copy.wait()
    for d in range(n):
        outs[d][plan.q_fl] = whole[d].astype(jnp.float32)
    even = chain_place("gy", plan.chain_y)[0]
    for d in range(n):
        start = lax.rem(me + d, n) * nx
        for x in range(nx):
            for k in range(5 + plan.n_state):
                q = state_index(plan, k - 5)
                up[0, k : k + 1] = outs[d][YM[k] if k < 5 else q, x, ny - 1 : ny]
                down[0, k : k + 1] = outs[d][YP[k] if k < 5 else q, x, 0:1]
            out_a[start + x] = pick(even, up[0], down[0])
            out_b[start + x] = pick(even, down[0], up[0])


def rows_kernel(plan, yr_a, yr_b, *outs):
    n = plan.n_gz
    me = lax.axis_index("gz")
    nx, half = plan.nx, plan.in_rows
    place = chain_place("gy", plan.chain_y)
    for d in range(n):
        start = lax.rem(me + d, n) * nx
        for x in range(-1, nx + 1):
            at = jnp.clip(start + x, 0, n * nx - 1)
            plus, minus = halo_pair(place, yr_a[at], yr_b[at])
            outs[d][x + 1, 0:half] = minus
            outs[d][x + 1, half : 2 * half] = plus


def tile_of(plan, refs, t, index):
    me = lax.axis_index("gz")
    out = refs[0][index]
    for d in range(1, plan.n_gz):
        out = pick(lax.rem(me - t + plan.n_gz, plan.n_gz) == d, refs[d][index], out)
    return out


def state_index(plan, k):
    if k < plan.steps:
        return plan.q_rho + k
    return plan.q_adh if k == plan.s_adh else plan.q_fl


def input_x_kernel(plan, *refs):
    n = plan.n_gz
    parts, rows, (out_a, out_b) = refs[:n], refs[n : 2 * n], refs[2 * n :]
    even = chain_place(X_AXES, plan.chain_x)[0]
    count, ny, half = 5 + plan.n_state, plan.ny, plan.in_rows
    for t in range(plan.tiles):
        for j in range(count):
            up = XM[j] if j < 5 else state_index(plan, j - 5)
            down = XP[j] if j < 5 else state_index(plan, j - 5)
            plus = tile_of(plan, parts, t, (up, plan.nx - 1))
            minus = tile_of(plan, parts, t, (down, 0))
            out_a[t, j * ny : (j + 1) * ny] = pick(even, plus, minus)
            out_b[t, j * ny : (j + 1) * ny] = pick(even, minus, plus)
        out_b[t, count * ny :] = jnp.zeros((plan.in_ends, plan.lanes), jnp.float32)
        upper = tile_of(plan, rows, t, (plan.nx,))
        lower = tile_of(plan, rows, t, (1,))
        r = count * ny
        for k in range(plan.n_state):
            for shift in (0, half):
                row = slice(shift + 5 + k, shift + 6 + k)
                out_b[t, r : r + 1] = pick(even, lower[row], upper[row])
                r += 1
        for shift, side, moving in ((0, -1, YM), (half, 1, YP)):
            row_up = shift + moving.index(EDGE[(-1, side)])
            row_low = shift + moving.index(EDGE[(1, side)])
            out_b[t, r : r + 1] = pick(even, lower[row_low : row_low + 1], upper[row_up : row_up + 1])
            r += 1


def fill_inputs(plan, parts, xr_a, xr_b, row_parts, state, apad):
    nx, ny, half = plan.nx, plan.ny, plan.in_rows
    count = 5 + plan.n_state
    place_x = chain_place(X_AXES, plan.chain_x)
    even, has_plus, has_minus = place_x
    own = slice(PAD, PAD + ny)
    first, last = slice(PAD - 1, PAD), slice(PAD + ny, PAD + ny + 1)
    fl = plan.s_fl
    for t in range(plan.tiles):
        near = [tile_of(plan, row_parts, t, (x,)) for x in range(nx + 2)]
        blank = jnp.zeros((1, plan.lanes), jnp.float32)

        def beyond(side, row, r):
            came = xr_b[t, count * ny + r : count * ny + r + 1]
            if side > 0:
                return pick(has_plus, pick(even, near[nx + 1][row : row + 1], came), blank)
            return pick(has_minus, pick(even, came, near[0][row : row + 1]), blank)

        for k in range(plan.n_state):
            rows = slice((5 + k) * ny, (6 + k) * ny)
            plus, minus = halo_pair(place_x, xr_a[t, rows], xr_b[t, rows])
            for x in range(-1, nx + 1):
                if x < 0:
                    plane = minus
                elif x == nx:
                    plane = plus
                else:
                    plane = tile_of(plan, parts, t, (state_index(plan, k), x))
                state[k, t, x + 1, own] = plane
                for shift, where, odd in ((0, first, 0), (half, last, 1)):
                    row = shift + 5 + k
                    if 0 <= x < nx:
                        value = near[x + 1][row : row + 1]
                    else:
                        value = beyond(-1 if x < 0 else 1, row, 2 * k + odd)
                    state[k, t, x + 1, where] = value
        for x in range(nx):
            mask = state[fl, t, x + 1, own]
            for i in range(19):
                apad[i, t, x + 1, own] = mask * tile_of(plan, parts, t, (i, x))
            mask_first = state[fl, t, x + 1, first]
            mask_last = state[fl, t, x + 1, last]
            for j in range(5):
                apad[YP[j], t, x + 1, last] = mask_last * near[x + 1][half + j : half + j + 1]
                apad[YM[j], t, x + 1, first] = mask_first * near[x + 1][j : j + 1]
        for j in range(5):
            rows = slice(j * ny, (j + 1) * ny)
            plus, minus = halo_pair(place_x, xr_a[t, rows], xr_b[t, rows])
            apad[XP[j], t, nx + 1, own] = state[fl, t, nx + 1, own] * plus
            apad[XM[j], t, 0, own] = state[fl, t, 0, own] * minus
        for side, where, shift, moving, odd in ((-1, first, 0, YM, 0), (1, last, half, YP, 1)):
            r = 2 * plan.n_state + odd
            low, high = EDGE[(-1, side)], EDGE[(1, side)]
            value = beyond(-1, shift + moving.index(low), r)
            apad[low, t, 0, where] = state[fl, t, 0, where] * value
            value = beyond(1, shift + moving.index(high), r)
            apad[high, t, nx + 1, where] = state[fl, t, nx + 1, where] * value


def complete_back(plan, last_phase, ksum, yr_a, yr_b, total):
    nx, ny = plan.nx, plan.ny
    lay = plan.y_layout(last_phase)
    place_y = chain_place("gy", plan.chain_y)
    total[...] = ksum[...]
    for t in range(plan.tiles):
        plus, minus = halo_pair(place_y, yr_a[t], yr_b[t])
        for x in range(nx + 2):
            r = lay["beyond"] + x
            rows = slice(PAD + ny - 1, PAD + ny)
            total[t, x, rows] = total[t, x, rows] + plus[r : r + 1]
            rows = slice(PAD, PAD + 1)
            total[t, x, rows] = total[t, x, rows] + minus[r : r + 1]
            if not last_phase:
                r = lay["own"] + x
                rows = slice(PAD + ny, PAD + ny + 1)
                total[t, x, rows] = total[t, x, rows] + plus[r : r + 1]
                rows = slice(PAD - 1, PAD)
                total[t, x, rows] = total[t, x, rows] + minus[r : r + 1]


def fill_next(plan, s, state, a_in, ksum, xr_a, xr_b, yr_a, yr_b, grad_in, grad_out, total, apad):
    nx, ny = plan.nx, plan.ny
    lay = plan.y_layout(False)
    place_x = chain_place(X_AXES, plan.chain_x)
    place_y = chain_place("gy", plan.chain_y)
    own = slice(PAD, PAD + ny)
    first, last = slice(PAD - 1, PAD), slice(PAD + ny, PAD + ny + 1)
    complete_back(plan, False, ksum, yr_a, yr_b, total)

    def extra(t, x, rows):
        mask = state[plan.s_fl, t, x + 1, rows]
        rho = state[s + 1, t, x + 1, rows]
        return (-COUPLING) * mask * jnp.exp(-rho) * total[t, x + 1, rows]

    for t in range(plan.tiles):
        y_plus, y_minus = halo_pair(place_y, yr_a[t], yr_b[t])
        for x in range(nx):
            more = extra(t, x, own)
            part = (1.0 - state[plan.s_fl, t, x + 1, own]) * total[t, x + 1, own]
            grad_out[t, x] = -part if grad_in is None else grad_in[t, x] - part
            for i in range(19):
                apad[i, t, x + 1, own] = a_in[i, t, x] + more
            more_first, more_last = extra(t, x, first), extra(t, x, last)
            for j in range(5):
                r = j * nx + x
                apad[YP[j], t, x + 1, last] = y_plus[r : r + 1] + more_last
                apad[YM[j], t, x + 1, first] = y_minus[r : r + 1] + more_first
        more_plus, more_minus = extra(t, nx, own), extra(t, -1, own)
        for j in range(5):
            rows = slice(j * ny, (j + 1) * ny)
            plus, minus = halo_pair(place_x, xr_a[t, rows], xr_b[t, rows])
            apad[XP[j], t, nx + 1, own] = plus + more_plus
            apad[XM[j], t, 0, own] = minus + more_minus
        r = lay["edges"]
        for side, rows, msg in ((1, last, y_plus), (-1, first, y_minus)):
            apad[EDGE[(-1, side)], t, 0, rows] = msg[r : r + 1] + extra(t, -1, rows)
            apad[EDGE[(1, side)], t, nx + 1, rows] = msg[r + 1 : r + 2] + extra(t, nx, rows)


def fill_phi(plan, s, state, phi):
    for t in range(plan.tiles):
        for x in range(plan.nx + 2):
            mask = state[plan.s_fl, t, x]
            psi = 1.0 - jnp.exp(-state[s, t, x])
            phi[t, x] = COUPLING * mask * psi + (1.0 - mask) * state[plan.s_adh, t, x]


def force_at(plan, phi, x, rows):
    tiles = range(plan.tiles)

    def at(dx, dy):
        return [phi[t, x + 1 + dx, rows.start + dy : rows.stop + dy] for t in tiles]

    sub, add = (lambda a, b: a - b), (lambda a, b: a + b)
    xp, xm, yp, ym, mid = at(1, 0), at(-1, 0), at(0, 1), at(0, -1), at(0, 0)
    pp, pm, mp, mm = at(1, 1), at(1, -1), at(-1, 1), at(-1, -1)
    dx, dy = each(sub, xp, xm), each(sub, yp, ym)
    zd = each(lambda m, a, b, c, d: C18 * m + C36 * ((a + b) + (c + d)), mid, xp, xm, yp, ym)
    dxu, dxd, dyu, dyd = z_shift(dx, 1), z_shift(dx, -1), z_shift(dy, 1), z_shift(dy, -1)
    px = each(
        lambda d, u, w, a, b, c, e: C18 * d + C36 * ((u + w) + ((a - c) + (b - e))),
        dx, dxu, dxd, pp, pm, mp, mm,
    )
    py = each(
        lambda d, u, w, a, b, c, e: C18 * d + C36 * ((u + w) + ((a - b) + (c - e))),
        dy, dyu, dyd, pp, pm, mp, mm,
    )
    pz = each(sub, z_shift(zd, 1), z_shift(zd, -1))
    return px, py, pz


def cells(plan, s, state, solid, fresh, vel, phi, apad, a_out, vpad, kept):
    nx, ny = plan.nx, plan.ny
    tiles = range(plan.tiles)
    for x in range(nx):
        for r0 in range(0, ny, 8):
            own = slice(PAD + r0, PAD + r0 + 8)
            here = slice(r0, r0 + 8)
            b = [[apad[0, t, x + 1, own] for t in tiles]]
            for i in range(1, 19):
                cx, cy, cz = DIRECTIONS[i]
                rows = slice(own.start + cy, own.stop + cy)
                came = [apad[i, t, x + 1 + cx, rows] for t in tiles]
                if cz:
                    came = z_shift(came, cz)
                if fresh:
                    open_to = [state[plan.s_fl, t, x + 1 + cx, rows] for t in tiles]
                    if cz:
                        open_to = z_shift(open_to, cz)
                    wall = [1.0 - v for v in open_to]
                    for t in tiles:
                        solid[i - 1, t, x, here] = wall[t]
                else:
                    wall = [solid[i - 1, t, x, here] for t in tiles]
                back = [apad[OPPOSITE[i], t, x + 1, own] for t in tiles]
                b.append(each(lambda c, w, o: c + w * o, came, wall, back))
            force = force_at(plan, phi, x, own)
            for t in tiles:
                g = [v[t] for v in b]
                sm = {i: g[i] + g[i + 1] for i in range(1, 19, 2)}
                df = {i: g[i] - g[i + 1] for i in range(1, 19, 2)}
                sxy, sxz, syz = sm[7] + sm[9], sm[11] + sm[13], sm[15] + sm[17]
                ux, uy, uz = vel(t, 0, x, here), vel(t, 1, x, here), vel(t, 2, x, here)
                m1x = W_AXIS * df[1] + W_DIAG * ((df[7] + df[9]) + (df[11] + df[13]))
                m1y = W_AXIS * df[3] + W_DIAG * ((df[7] - df[9]) + (df[15] + df[17]))
                m1z = W_AXIS * df[5] + W_DIAG * ((df[11] - df[13]) + (df[15] - df[17]))
                mxx = W_AXIS * sm[1] + W_DIAG * (sxy + sxz)
                myy = W_AXIS * sm[3] + W_DIAG * (sxy + syz)
                mzz = W_AXIS * sm[5] + W_DIAG * (sxz + syz)
                mxy = W_DIAG * (sm[7] - sm[9])
                mxz = W_DIAG * (sm[11] - sm[13])
                myz = W_DIAG * (sm[15] - sm[17])
                m0 = W_REST * g[0] + W_AXIS * ((sm[1] + sm[3]) + sm[5]) + W_DIAG * ((sxy + sxz) + syz)
                vx = mxx * ux + mxy * uy + mxz * uz
                vy = mxy * ux + myy * uy + myz * uz
                vz = mxz * ux + myz * uy + mzz * uz
                mbx = 3.0 * (m1x - ux * m0) + 9.0 * vx
                mby = 3.0 * (m1y - uy * m0) + 9.0 * vy
                mbz = 3.0 * (m1z - uz * m0) + 9.0 * vz
                usq = ux * ux + uy * uy + uz * uz
                rhobar = m0 * (1.0 + 1.5 * usq) - 4.5 * (ux * vx + uy * vy + uz * vz)
                fade = jnp.exp(-state[s, t, x + 1, own])
                mask = state[plan.s_fl, t, x + 1, own]
                pull = mbx * force[0][t] + mby * force[1][t] + mbz * force[2][t]
                rhobar = rhobar - RELAX_TIME * pull * fade
                scale = RELAX_TIME * mask * (1.0 - fade)
                vpad[0, t, x, own] = scale * mbx
                vpad[1, t, x, own] = scale * mby
                vpad[2, t, x, own] = scale * mbz
                rb, mx, my, mz = mask * rhobar, mask * mbx, mask * mby, mask * mbz
                damp = (1.0 - 1.0 / RELAX_TIME) * mask
                a_out(0, t, x, here, rb + damp * g[0])
                for i in range(1, 19, 2):
                    cx, cy, cz = DIRECTIONS[i]
                    along = None
                    for c, m in ((cx, mx), (cy, my), (cz, mz)):
                        if c == 1:
                            along = m if along is None else along + m
                        elif c == -1:
                            along = along - m
                    a_out(i, t, x, here, (rb + along) + damp * g[i])
                    a_out(i + 1, t, x, here, (rb - along) + damp * g[i + 1])


def sums_of_back(plan, vpad, kext):
    nx, ny = plan.nx, plan.ny
    tiles = range(plan.tiles)
    add = lambda a, b: a + b
    chunks = [slice(PAD + r, PAD + r + 8) for r in range(0, ny, 8)]
    chunks += [slice(PAD - 1, PAD), slice(PAD + ny, PAD + ny + 1)]
    for x in range(-1, nx + 1):
        for rows in chunks:

            def at(k, dx, dy):
                if not 0 <= x + dx < nx:
                    return None
                return [vpad[k, t, x + dx, rows.start + dy : rows.stop + dy] for t in tiles]

            def combine(a, b, sign):
                if a is None and b is None:
                    return None
                if b is None:
                    return a
                if a is None:
                    return b if sign > 0 else [-v for v in b]
                return each((lambda p, q: p + q) if sign > 0 else (lambda p, q: p - q), a, b)

            def times(c, a):
                return None if a is None else [c * v for v in a]

            dx0 = combine(at(0, 1, 0), at(0, -1, 0), -1)
            dxs = combine(
                combine(at(0, 1, 1), at(0, -1, 1), -1), combine(at(0, 1, -1), at(0, -1, -1), -1), 1
            )
            dy0 = combine(at(1, 0, 1), at(1, 0, -1), -1)
            dys = combine(
                combine(at(1, 1, 1), at(1, 1, -1), -1), combine(at(1, -1, 1), at(1, -1, -1), -1), 1
            )
            zsum = times(C36, combine(dx0, dy0, 1))
            side = combine(combine(at(2, 1, 0), at(2, -1, 0), 1), combine(at(2, 0, 1), at(2, 0, -1), 1), 1)
            zdif = combine(times(C18, at(2, 0, 0)), times(C36, side), 1)
            flat = combine(times(C18, combine(dx0, dy0, 1)), times(C36, combine(dxs, dys, 1)), 1)
            up = z_shift(combine(zsum, zdif, 1), 1)
            down = z_shift(combine(zsum, zdif, -1), -1)
            for t in tiles:
                kext[t, x + 1, rows] = -(flat[t] + (up[t] + down[t]))


def pack_x(plan, last_phase, a_of, kext, out_a, out_b):
    nx, ny = plan.nx, plan.ny
    lay = plan.x_layout(last_phase)
    even = chain_place(X_AXES, plan.chain_x)[0]
    own = slice(PAD, PAD + ny)

    def put(t, rows, plus, minus):
        out_a[t, rows] = pick(even, plus, minus)
        out_b[t, rows] = pick(even, minus, plus)

    for t in range(plan.tiles):
        if not last_phase:
            for j in range(5):
                put(t, slice(j * ny, (j + 1) * ny), a_of(XM[j], t, nx - 1), a_of(XP[j], t, 0))
            put(t, slice(lay["own"], lay["own"] + ny), kext[t, nx, own], kext[t, 1, own])
        put(t, slice(lay["beyond"], lay["beyond"] + ny), kext[t, nx + 1, own], kext[t, 0, own])
        r = lay["ends"]
        blank = jnp.zeros((8, plan.lanes), jnp.float32)
        out_a[t, r : r + 8] = blank
        out_b[t, r : r + 8] = blank
        for j, row in enumerate((PAD - 1, PAD + ny)):
            rows = slice(row, row + 1)
            put(t, slice(r + j, r + j + 1), kext[t, nx + 1, rows], kext[t, 0, rows])
            if not last_phase:
                put(t, slice(r + 2 + j, r + 3 + j), kext[t, nx, rows], kext[t, 1, rows])


def pack_rows(plan, a_of_row, up, down):
    for t in range(plan.tiles):
        up[t] = jnp.zeros_like(up[t])
        down[t] = jnp.zeros_like(down[t])
        for j in range(5):
            for x in range(plan.nx):
                r = j * plan.nx + x
                up[t, r : r + 1] = a_of_row(YM[j], t, x, plan.ny - 1)
                down[t, r : r + 1] = a_of_row(YP[j], t, x, 0)


def finish_step(plan, last_phase, a_ref, vpad, kext, out_a, out_b, up, down):
    sums_of_back(plan, vpad, kext)
    pack_x(plan, last_phase, lambda i, t, x: a_ref[i, t, x], kext, out_a, out_b)
    if not last_phase:
        pack_rows(plan, lambda i, t, x, row: a_ref[i, t, x, row : row + 1], up, down)


def blank_rows(plan, ref):
    blank = jnp.zeros((PAD, plan.lanes), jnp.float32)
    for k in range(3):
        for t in range(plan.tiles):
            for x in range(plan.nx):
                ref[k, t, x, 0:PAD] = blank
                ref[k, t, x, PAD + plan.ny :] = blank


def first_kernel(plan, *refs):
    n = plan.n_gz
    parts, row_parts, (xr_a, xr_b) = refs[:n], refs[n : 2 * n], refs[2 * n : 2 * n + 2]
    state, solid, vels, a_ref, kext, out_a, out_b, up, down, apad, phi, vpad = refs[2 * n + 2 :]
    s = plan.steps - 1
    last_phase = s == 0
    fill_inputs(plan, parts, xr_a, xr_b, row_parts, state, apad)
    for t in range(plan.tiles):
        for k in range(3 * (plan.steps - 1)):
            vels[k, t] = tile_of(plan, parts, t, (plan.q_vel + k,))
    fill_phi(plan, s, state, phi)
    blank_rows(plan, vpad)

    def vel(t, k, x, here):
        return tile_of(plan, parts, t, (plan.q_vel + 3 * s + k, x, here))

    def a_out(i, t, x, here, value):
        a_ref[i, t, x, here] = value

    cells(plan, s, state, solid, True, vel, phi, apad, a_out, vpad, None)
    finish_step(plan, last_phase, a_ref, vpad, kext, out_a, out_b, up, down)


def next_kernel(plan, s, has_grad, *refs):
    refs = list(refs)
    take = lambda k: [refs.pop(0) for _ in range(k)]
    last_phase = s == 0
    state, solid, vels, a_in, ksum, xr_a, xr_b, yr_a, yr_b = take(9)
    grad_in = take(1)[0] if has_grad else None
    if last_phase:
        tiles_out = take(plan.n_gz)
        kext, out_a, out_b, grad_out, apad, phi, vpad, total, a_ref = take(9)
        up = down = None
    else:
        a_ref, kext, out_a, out_b, up, down, grad_out, apad, phi, vpad, total = take(11)
    fill_next(plan, s, state, a_in, ksum, xr_a, xr_b, yr_a, yr_b, grad_in, grad_out, total, apad)
    fill_phi(plan, s, state, phi)
    blank_rows(plan, vpad)

    def vel(t, k, x, here):
        return vels[3 * s + k, t, x, here]

    def a_out(i, t, x, here, value):
        if last_phase:
            a_ref[t, i, x, here] = value
        else:
            a_ref[i, t, x, here] = value

    cells(plan, s, state, solid, False, vel, phi, apad, a_out, vpad, None)
    finish_step(plan, last_phase, a_ref, vpad, kext, out_a, out_b, up, down)
    if last_phase:
        me = lax.axis_index("gz")
        for d in range(plan.n_gz):
            tiles_out[d][...] = a_ref[lax.rem(me + d, plan.n_gz)]


def y_kernel(plan, last_phase, *refs):
    if last_phase:
        kext, xr_a, xr_b, ksum, out_a, out_b, up, down = refs
        up[...] = jnp.zeros_like(up)
        down[...] = jnp.zeros_like(down)
    else:
        kext, xr_a, xr_b, up_in, down_in, ksum, out_a, out_b, up, down = refs
        up[...] = up_in[...]
        down[...] = down_in[...]
    nx, ny = plan.nx, plan.ny
    lay_x, lay_y = plan.x_layout(last_phase), plan.y_layout(last_phase)
    place_x = chain_place(X_AXES, plan.chain_x)
    even = chain_place("gy", plan.chain_y)[0]
    own = slice(PAD, PAD + ny)
    ksum[...] = kext[...]
    for t in range(plan.tiles):

        def add(x, rows, msg_rows, side):
            part = halo_pair(place_x, xr_a[t, msg_rows], xr_b[t, msg_rows])[side]
            ksum[t, x + 1, rows] = ksum[t, x + 1, rows] + part

        for x, side in ((nx - 1, 0), (0, 1)):
            add(x, own, slice(lay_x["beyond"], lay_x["beyond"] + ny), side)
            for j, row in enumerate((PAD - 1, PAD + ny)):
                r = lay_x["ends"] + j
                add(x, slice(row, row + 1), slice(r, r + 1), side)
        if not last_phase:
            for x, side in ((nx, 0), (-1, 1)):
                add(x, own, slice(lay_x["own"], lay_x["own"] + ny), side)
                for j, row in enumerate((PAD - 1, PAD + ny)):
                    r = lay_x["ends"] + 2 + j
                    add(x, slice(row, row + 1), slice(r, r + 1), side)
            r = lay_y["edges"]
            for side, out, row in ((-1, up, ny - 1), (1, down, 0)):
                j = XM.index(EDGE[(-1, side)]) * ny + row
                out[t, r : r + 1] = halo_pair(place_x, xr_a[t, j : j + 1], xr_b[t, j : j + 1])[1]
                j = XP.index(EDGE[(1, side)]) * ny + row
                out[t, r + 1 : r + 2] = halo_pair(place_x, xr_a[t, j : j + 1], xr_b[t, j : j + 1])[0]
        for x in range(nx + 2):
            r = lay_y["beyond"] + x
            up[t, r : r + 1] = ksum[t, x, PAD + ny : PAD + ny + 1]
            down[t, r : r + 1] = ksum[t, x, PAD - 1 : PAD]
            if not last_phase:
                r = lay_y["own"] + x
                up[t, r : r + 1] = ksum[t, x, PAD + ny - 1 : PAD + ny]
                down[t, r : r + 1] = ksum[t, x, PAD : PAD + 1]
        out_a[t] = pick(even, up[t], down[t])
        out_b[t] = pick(even, down[t], up[t])


def close_kernel(plan, state, ksum, yr_a, yr_b, grad_in, *rest):
    n = plan.n_gz
    outs, (total, both) = rest[:n], rest[n:]
    own = slice(PAD, PAD + plan.ny)
    complete_back(plan, True, ksum, yr_a, yr_b, total)
    for t in range(plan.tiles):
        for x in range(plan.nx):
            mask = state[plan.s_fl, t, x + 1, own]
            rho = state[0, t, x + 1, own]
            back = total[t, x + 1, own]
            both[t, 0, x] = (-COUPLING) * mask * jnp.exp(-rho) * back
            both[t, 1, x] = grad_in[t, x] - (1.0 - mask) * back
    me = lax.axis_index("gz")
    for d in range(n):
        outs[d][...] = both[lax.rem(me + d, n)]


def join_kernel(plan, *refs):
    n = plan.n_gz
    a_parts, r_parts, (out, grad) = refs[:n], refs[n : 2 * n], refs[2 * n :]
    me = lax.axis_index("gz")
    for d in range(n):
        chunk = pl.ds(lax.rem(me - d + n, n) * plan.nx, plan.nx)
        for i in range(19):
            out[i, chunk] = a_parts[d][i] + r_parts[d][0]
        grad[chunk] = r_parts[d][1]


def swap_pairs(plan, along_gy, odd):
    n_gx, n_gy, n_gz = plan.n_gx, plan.n_gy, plan.n_gz
    out = []
    for x in range(n_gx):
        for y in range(n_gy):
            for z in range(n_gz):
                place, count = (y, n_gy) if along_gy else (x * n_gz + z, n_gx * n_gz)
                other = place + 1 if place % 2 == odd else place - 1
                to = (x, y, z)
                if 0 <= other < count:
                    to = (x, other, z) if along_gy else (other // n_gz, y, other % n_gz)
                elif along_gy and n_gz % 2 == 0:
                    to = (x, y, z ^ 1)
                elif not along_gy and n_gy % 2 == 0:
                    to = (x, y ^ 1, z)
                out.append(((x * n_gy + y) * n_gz + z, (to[0] * n_gy + to[1]) * n_gz + to[2]))
    return out


def swap_along(plan, along_gy, first, second):
    axes = ("gx", "gy", "gz")
    late = lax.ppermute(second, axes, swap_pairs(plan, along_gy, 1))
    return lax.ppermute(first, axes, swap_pairs(plan, along_gy, 0)), late


def call(kernel, name, outs, scratch, args, flops, in_hbm=False):
    spec = pl.BlockSpec(memory_space=pltpu.HBM if in_hbm else pltpu.VMEM)
    return pl.pallas_call(
        kernel,
        name=name,
        out_shape=tuple(jax.ShapeDtypeStruct(shape, jnp.float32) for shape in outs),
        in_specs=[spec] * len(args),
        out_specs=tuple(pl.BlockSpec(memory_space=pltpu.VMEM) for _ in outs),
        scratch_shapes=scratch,
        cost_estimate=pl.CostEstimate(flops=flops, bytes_accessed=0, transcendentals=0),
        compiler_params=pltpu.CompilerParams(vmem_limit_bytes=VMEM_LIMIT),
    )(*[pltpu.with_memory_space_constraint(v, pltpu.HBM) if in_hbm else v for v in args])


def per_device(cotangent, densities, velocities, adhesion, fluid):
    n = lax.axis_size("gz")
    plan = Plan(lax.axis_size("gx"), lax.axis_size("gy"), n, adhesion.shape, densities.shape[0])
    tiles, nx, ny, lanes, steps = plan.tiles, plan.nx, plan.ny, plan.lanes, plan.steps
    f32 = jnp.float32
    field = (tiles, nx, ny, lanes)
    padded = plan.padded(1)[1:]

    def along_x(first, second):
        return swap_along(plan, False, first, second)

    def along_y(first, second):
        return swap_along(plan, True, first, second)

    def within_gz(parts):
        return [parts[0]] + [
            lax.ppermute(parts[d], "gz", [(i, (i + d) % n) for i in range(n)]) for d in range(1, n)
        ]

    part = (plan.nq, nx, ny, lanes)
    half = plan.in_rows
    msg = (n * nx, half, lanes)
    scratch = [pltpu.VMEM((n, nx, ny, lanes), jnp.int32)] + [pltpu.VMEM((1, half, lanes), f32)] * 2
    *parts, ya, yb = call(
        functools.partial(split_kernel, plan),
        "split",
        [part] * n + [msg] * 2,
        scratch + [pltpu.SemaphoreType.DMA((n, 4 + steps))],
        (cotangent, densities, velocities, adhesion, fluid),
        1000,
        in_hbm=True,
    )
    parts = within_gz(parts)
    yr = along_y(ya, yb)
    msg = (nx + 2, 2 * half, lanes)
    row_parts = within_gz(call(functools.partial(rows_kernel, plan), "rows_in", [msg] * n, [], yr, 1000))
    count = (5 + plan.n_state) * ny
    msgs = [(tiles, count, lanes), (tiles, count + plan.in_ends, lanes)]
    xr = along_x(
        *call(functools.partial(input_x_kernel, plan), "input_x", msgs, [], (*parts, *row_parts), 1000)
    )

    work = [pltpu.VMEM(plan.padded(19), f32), pltpu.VMEM(padded, f32)]
    work.append(pltpu.VMEM((3, tiles, nx, plan.rows, lanes), f32))

    def x_message(last_phase):
        return (tiles, plan.x_layout(last_phase)["rows"], lanes)

    def y_message(last_phase):
        return (tiles, plan.y_layout(last_phase)["rows"], lanes)

    pops = (19, *field)
    outs = [plan.padded(plan.n_state), (18, *field), (3 * (steps - 1), *field), pops, padded]
    outs += [x_message(False)] * 2 + [y_message(False)] * 2
    state, solid, vels, a, kext, xa, xb, up, down = call(
        functools.partial(first_kernel, plan), "first", outs, work, (*parts, *row_parts, *xr), 100000
    )
    grad = None
    for s in reversed(range(steps - 1)):
        xr = along_x(xa, xb)
        msg = y_message(False)
        ksum, ya, yb = call(
            functools.partial(y_kernel, plan, False),
            f"rows_{s}",
            [padded, msg, msg],
            [pltpu.VMEM(msg, f32)] * 2,
            (kext, *xr, up, down),
            1000,
        )
        yr = along_y(ya, yb)
        args = [state, solid, vels, a, ksum, *xr, *yr]
        if grad is not None:
            args.append(grad)
        scratch = work + [pltpu.VMEM(padded, f32)]
        if s > 0:
            outs = [pops, padded] + [x_message(False)] * 2 + [y_message(False)] * 2 + [field]
        else:
            outs = [(19, nx, ny, lanes)] * n + [padded] + [x_message(True)] * 2 + [field]
            scratch = scratch + [pltpu.VMEM((tiles, 19, nx, ny, lanes), f32)]
        res = call(
            functools.partial(next_kernel, plan, s, grad is not None), f"next_{s}", outs, scratch, args, 100000
        )
        if s > 0:
            a, kext, xa, xb, up, down, grad = res
        else:
            a_parts, (kext, xa, xb, grad) = res[:n], res[n:]

    a_parts = within_gz(a_parts)
    xr = along_x(xa, xb)
    msg = y_message(True)
    ksum, ya, yb = call(
        functools.partial(y_kernel, plan, True),
        "rows_end",
        [padded, msg, msg],
        [pltpu.VMEM(msg, f32)] * 2,
        (kext, *xr),
        1000,
    )
    yr = along_y(ya, yb)
    both = (2, nx, ny, lanes)
    r_parts = call(
        functools.partial(close_kernel, plan),
        "close",
        [both] * n,
        [pltpu.VMEM(padded, f32), pltpu.VMEM((tiles, *both), f32)],
        (state, ksum, *yr, grad),
        1000,
    )
    r_parts = within_gz(r_parts)
    out, gradient = call(
        functools.partial(join_kernel, plan),
        "join",
        [cotangent.shape, adhesion.shape],
        [],
        (*a_parts, *r_parts),
        1000,
    )
    return out, gradient


def solution(mesh):
    return jax.shard_map(
        per_device,
        mesh=mesh,
        in_specs=(
            P(None, "gx", "gy", "gz"),
            P(None, "gx", "gy", "gz"),
            P(None, None, "gx", "gy", "gz"),
            P("gx", "gy", "gz"),
            P("gx", "gy", "gz"),
        ),
        out_specs=(P(None, "gx", "gy", "gz"), P("gx", "gy", "gz")),
        check_vma=False,
    )
```
